32 devices in a mesh: ctx: 8 (over z, y), head: 4 (over x, core).
Axes of the slice: x: 2, y: 2, z: 4, core: 2. Of those that a mesh axis runs over, the one named last changes fastest.
Arguments:
- hidden: bfloat16 [1024, 4096], P('ctx', 'head'), may hold values from -6 to 6
- w_proj: bfloat16 [4096, 1024], P('head'), may hold values from -0.125 to 0.125
- b_proj: bfloat16 [4096, 8], P('head'), may hold values from -0.09375 to 0.09375
- queries: bfloat16 [1024, 4096], P('ctx', 'head'), may hold values from -300 to 300
- keys: bfloat16 [1024, 1024], P('ctx', 'head'), may hold values from -6 to 6
- values: bfloat16 [1024, 1024], P('ctx', 'head'), may hold values from -6 to 6
- reach: int32 [8], P('ctx'), may hold values from 1 to 5
Outputs:
- numer: float32 [1024, 4096], P('ctx', 'head')
- totals: float32 [32, 1024], P('head', 'ctx')
- maxima: float32 [32, 1024], P('head', 'ctx')
- carried: bfloat16 [1024, 4096], P('ctx', 'head')
The draws below stay inside these ranges and needn't reach their ends.
All inputs are finite; a program needn't handle non-finite values.
Results may differ from the reference program's by a relative error of at most 0.0064.
Values may be sent and summed in bfloat16 or wider, within the bound.
A program may use at most 64 MiB of HBM per device.

```python
import jax
import jax.numpy as jnp
from jax import lax

D = 4096
HQ = 32
KVH = 8
HD = 128
TOK_DEV = 128
STEPS = 5
TOKENS = 1024
N_CTX = 8


def draw_queries(key, part):
    base = jax.random.normal(key, (TOKENS, HQ * HD), jnp.float32)
    return jnp.clip(base, -300.0, 300.0).astype(jnp.bfloat16)


def set_ends(drawn, stream_key, low, high):
    index_at = [jax.random.randint(jax.random.fold_in(stream_key, axis), (), 0, length) for axis, length in enumerate(drawn.shape)]
    longest = drawn.shape.index(max(drawn.shape))
    neighbour = index_at[:longest] + [(index_at[longest] + 1) % drawn.shape[longest]] + index_at[longest + 1:]
    return drawn.at[tuple(index_at)].set(low).at[tuple(neighbour)].set(high)


def raised(entries, stream_key, source, target, blocks, factor):
    owner, partner = [(jnp.arange(entries.shape[axis_at]) // (entries.shape[axis_at] // blocks)).reshape([-1 if axis == axis_at else 1 for axis in range(entries.ndim)]) for axis_at in (source, target)]
    chosen = jax.random.permutation(stream_key, blocks)[partner]
    strong = (owner == chosen) | (owner == (partner + blocks // 2) % blocks)
    return jnp.where(strong, factor * entries, entries)


def level_of(key, shape, pieces, smallest, high):
    level = 1.0
    for dim, parts in pieces:
        steps = jax.random.uniform(jax.random.fold_in(jax.random.fold_in(key, 6), dim), (parts,), jnp.float32, smallest / len(pieces), high / len(pieces))
        level = level * jnp.repeat(jnp.exp(steps), shape[dim] // parts).reshape((-1,) + (1,) * (len(shape) - 1 - dim))
    return level


def bell_draw(stream_key, shape, width, most, pieces=(), kind=jnp.bfloat16):
    values = jax.random.normal(stream_key, shape, jnp.float32) * width
    if len(pieces) > 0:
        values = level_of(stream_key, shape, pieces, -0.22, 0.18) * values
    return jnp.clip(values, min=-most, max=most).astype(kind)


def heavy_noise(rng, extent, deviation, limit, split, heavy, kind=jnp.bfloat16):
    entries = deviation * jax.random.normal(rng, extent, jnp.float32)
    if split:
        entries = entries * level_of(rng, extent, split, -0.22, 0.18)
    return jnp.clip(raised(entries, jax.random.fold_in(rng, 3), *heavy), -limit, limit).astype(kind)


def setup_inputs(seed: int = 0) -> dict:
    streams_of = jax.random.split(jax.random.key(seed), 8)
    return {
        "hidden": bell_draw(streams_of[0], (TOKENS, D), 1.0, 6.0, ((0, 8), (1, 4))),
        "w_proj": heavy_noise(streams_of[1], (D, KVH * HD), D ** -0.5, 0.125, ((0, 4),), (0, 1, 4, 2.0)),
        "b_proj": bell_draw(streams_of[2], (D, KVH), D ** -0.5, 0.09375, ((0, 4),)),
        "queries": draw_queries(jax.random.fold_in(streams_of[7], 71), 0),
        "keys": bell_draw(streams_of[4], (TOKENS, KVH * HD), 1.0, 6.0, ((0, 8), (1, 4))),
        "values": bell_draw(streams_of[5], (TOKENS, KVH * HD), 1.0, 6.0, ((0, 8), (1, 4))),
        "reach": set_ends(jax.random.randint(streams_of[6], (N_CTX,), 1, STEPS + 1), jax.random.fold_in(streams_of[6], 1), 1, STEPS).astype(jnp.int32),
    }


very_low = -1e+30
highest = lax.Precision.HIGHEST

def transitions(raw_dirs, logits):
    vectors = raw_dirs * lax.rsqrt(lax.optimization_barrier(jnp.sum(raw_dirs * raw_dirs, axis=-1, keepdims=True)) + 1e-06)
    beta_vals = 2.0 / (1.0 + jnp.exp(-logits))
    gram_mat = jnp.einsum('hte,hue->htu', vectors, vectors, precision=highest)
    length = vectors.shape[1]
    identity = jnp.eye(length, dtype=vectors.dtype)
    lower_mat = identity[None] + beta_vals[:, :, None] * jnp.tril(gram_mat, -1)
    diag_beta = identity[None] * beta_vals[:, None, :]
    triangle = lax.linalg.triangular_solve(lower_mat, diag_beta, left_side=True, lower=True, unit_diagonal=True)
    return (vectors, triangle)

def key_terms(vectors, triangle, key_float):
    key_tri = jnp.triu(jnp.einsum('hue,hje->huj', vectors, key_float, precision=highest), 1)
    key_mix = jnp.einsum('htu,huj->htj', triangle, key_tri, precision=highest)
    keys_moved = (key_float - jnp.einsum('htj,hte->hje', key_mix, vectors, precision=highest)).astype(jnp.bfloat16)
    identity = jnp.eye(vectors.shape[2], dtype=vectors.dtype)
    block_prod = identity[None] - jnp.einsum('hte,htu,huf->hef', vectors, triangle, vectors, precision=highest)
    return (keys_moved, block_prod, key_tri)

def query_terms(vectors, triangle, query_float):
    query_vec = jnp.tril(jnp.einsum('hgie,hte->hgit', query_float, vectors, precision=highest))
    query_tri = jnp.einsum('hgit,htu->hgiu', query_vec, triangle, precision=highest)
    query_hat = query_float - jnp.einsum('hgiu,hue->hgie', query_tri, vectors, precision=highest)
    return (query_hat, query_tri)

def reference(hidden, w_proj, b_proj, queries, keys, values, reach):
    blocks = N_CTX
    length = TOK_DEV
    head_dim = HD
    groups = HQ // KVH
    scaling = head_dim ** (-0.5)
    raw_all = jnp.dot(hidden.astype(jnp.float32), w_proj.astype(jnp.float32), preferred_element_type=jnp.float32)
    raw_all = raw_all.reshape(blocks, length, KVH, head_dim).transpose(0, 2, 1, 3)
    logit_all = jnp.dot(hidden.astype(jnp.float32), b_proj.astype(jnp.float32), preferred_element_type=jnp.float32)
    logit_all = logit_all.reshape(blocks, length, KVH).transpose(0, 2, 1)
    key_blocks = keys.reshape(blocks, length, KVH, head_dim).transpose(0, 2, 1, 3)
    value_blocks = values.reshape(blocks, length, KVH, head_dim).transpose(0, 2, 1, 3)
    query_blocks = queries.reshape(blocks, length, KVH, groups, head_dim).transpose(0, 2, 3, 1, 4)

    def key_section(inputs):
        raw_dirs, logits, key_block = inputs
        vectors, triangle = transitions(raw_dirs, logits)
        keys_moved, block_prod, key_tri = key_terms(vectors, triangle, key_block.astype(jnp.float32))
        return (keys_moved, block_prod)
    moved_all, prod_all = lax.map(key_section, (raw_all, logit_all, key_blocks))
    causal = jnp.arange(length)[:, None] >= jnp.arange(length)[None, :]
    identity = jnp.eye(head_dim, dtype=jnp.float32)

    def query_section(inputs):
        block_id, raw_dirs, logits, key_block, query_block, reach_now = inputs
        vectors, triangle = transitions(raw_dirs, logits)
        key_float = key_block.astype(jnp.float32)
        query_float = query_block.astype(jnp.float32)
        unused_keys, unused_prod, key_tri = key_terms(vectors, triangle, key_float)
        query_hat, query_tri = query_terms(vectors, triangle, query_float)
        own = jnp.einsum('hgie,hje->hgij', query_float, key_float, precision=highest)
        own = own - jnp.einsum('hgiu,huj->hgij', query_tri, key_tri, precision=highest)
        own = jnp.where(causal, own * scaling, very_low)
        score_list = [own]
        value_list = [value_blocks[block_id].astype(jnp.float32)]
        carried_q = query_hat
        for offset in range(1, STEPS):
            source = block_id - offset
            clamped = jnp.maximum(source, 0).astype(jnp.int32)
            is_live = jnp.logical_and(offset < reach_now, source >= 0)
            rounded = carried_q.astype(jnp.bfloat16).astype(jnp.float32)
            scores = jnp.einsum('hgie,hje->hgij', rounded, moved_all[clamped].astype(jnp.float32), precision=highest) * scaling
            score_list.append(jnp.where(is_live, scores, very_low))
            value_list.append(value_blocks[clamped].astype(jnp.float32))
            step_prod = jnp.where(source >= 0, prod_all[clamped], identity[None])
            carried_q = jnp.einsum('hgie,hef->hgif', carried_q, step_prod, precision=highest)
        stacked = jnp.stack(score_list)
        row_max = lax.optimization_barrier(jnp.max(lax.optimization_barrier(jnp.max(stacked, axis=-1)), axis=0))
        probs = jnp.exp(stacked - row_max[None, :, :, :, None])
        sums = lax.optimization_barrier(jnp.sum(lax.optimization_barrier(jnp.sum(probs, axis=-1)), axis=0))
        rounded_p = probs.astype(jnp.bfloat16).astype(jnp.float32)
        numer_acc = jnp.zeros_like(query_hat)
        for offset in range(STEPS):
            numer_acc = numer_acc + jnp.einsum('hgij,hje->hgie', rounded_p[offset], value_list[offset], precision=highest)
        return (numer_acc, sums, row_max, carried_q.astype(jnp.bfloat16))
    block_ids = jnp.arange(blocks, dtype=jnp.int32)
    numer_b, sums_b, max_b, carry_b = lax.map(query_section, (block_ids, raw_all, logit_all, key_blocks, query_blocks, reach))
    numer = numer_b.transpose(0, 3, 1, 2, 4).reshape(blocks * length, HQ * head_dim)
    totals = sums_b.transpose(1, 2, 0, 3).reshape(HQ, blocks * length)
    maxima = max_b.transpose(1, 2, 0, 3).reshape(HQ, blocks * length)
    carried = carry_b.transpose(0, 3, 1, 2, 4).reshape(blocks * length, HQ * head_dim)
    return (numer, totals, maxima, carried)
```

```python
import functools

import jax
import jax.numpy as jnp
from jax import lax
from jax.experimental import pallas as pl
from jax.experimental.pallas import tpu as pltpu
from jax.sharding import PartitionSpec as P

STEPS = 5
FAR = jnp.float32
PROD_PARTS = 2

very_low = -1e30
f32 = jnp.float32
bf16 = jnp.bfloat16
MESH = pl.DeviceIdType.MESH


def dot(a, b):
    return lax.dot_general(a, b, (((1,), (0,)), ((), ())), preferred_element_type=f32)


def dot_t(a, b):
    return lax.dot_general(a, b, (((1,), (1,)), ((), ())), preferred_element_type=f32)


def split(x):
    high = x.astype(bf16)
    return high, (x - high.astype(f32)).astype(bf16)


def halves(x):
    n = x.shape[1] // 2
    return x[:, :n] + x[:, n:]


def wide(x):
    return jnp.concatenate(split(x), axis=1)


def mm(a, b):
    both = wide(b)
    return halves(dot(wide(a), jnp.concatenate([both, both], axis=0)))


def mm_t(a, b):
    high, low = split(b)
    rhs = jnp.concatenate(
        [jnp.concatenate([high, high], axis=1), jnp.concatenate([low, low], axis=1)], axis=0
    )
    return halves(dot_t(wide(a), rhs))


def exact_mm_t(a, b):
    return halves(dot_t(a, jnp.concatenate(split(b), axis=0)))


def kernel(
    n_head, n_ctx,
    hid_hbm, w_hbm, b_hbm, q_hbm, k_hbm, v_hbm, reach,
    numer, totals, maxima, carried,
    hid, w, b, q, k, part, got, plog, glog, lsum, vals, bun, carry, score, qvec,
    local_sem, w_sem, part_send, part_recv, log_send, log_recv,
    val_send, val_recv, bun_send, bun_recv,
):
    me = lax.axis_index("head")
    ctx = lax.axis_index("ctx")
    parity = lax.rem(ctx, 2)
    partner = ctx + 1 - 2 * parity
    length = hid.shape[0]
    kv_heads = bun.shape[1]
    head_dim = bun.shape[3]
    groups = q.shape[1] // (kv_heads * head_dim)
    columns = kv_heads * head_dim
    scaling = head_dim ** (-0.5)
    others = sorted(range(1, n_head), key=lambda i: abs(i - n_head // 2))

    barrier = pltpu.get_barrier_semaphore()
    for i in others:
        pl.semaphore_signal(
            barrier, inc=1, device_id={"head": lax.rem(me + i, n_head)}, device_id_type=MESH
        )
    pl.semaphore_signal(barrier, inc=1, device_id={"ctx": partner}, device_id_type=MESH)
    has_next, has_last = ctx + 2 < n_ctx, ctx >= 2

    @pl.when(has_next)
    def _():
        pl.semaphore_signal(barrier, inc=1, device_id={"ctx": ctx + 2}, device_id_type=MESH)

    @pl.when(has_last)
    def _():
        pl.semaphore_signal(barrier, inc=1, device_id={"ctx": ctx - 2}, device_id_type=MESH)

    def local(src, dst, sem):
        copy = pltpu.make_async_copy(src, dst, sem)
        copy.start()
        return copy

    hid_in = local(hid_hbm, hid, local_sem.at[0])
    b_in = local(b_hbm, b, local_sem.at[1])
    w_in = []
    for i in others + [0]:
        at = pl.multiple_of(lax.rem(me + i, n_head) * columns, columns)
        w_in.append(local(w_hbm.at[:, pl.ds(at, columns)], w.at[i], w_sem.at[i]))
    v_in = local(v_hbm, vals.at[0], local_sem.at[2])
    k_in = local(k_hbm, k, local_sem.at[3])
    q_in = local(q_hbm, q, local_sem.at[4])

    row = lax.broadcasted_iota(jnp.int32, (length, length), 0)
    col = lax.broadcasted_iota(jnp.int32, (length, length), 1)
    eye = jnp.where(row == col, 1.0, 0.0).astype(f32)

    for s in range(1, STEPS):
        @pl.when(ctx < s)
        def _():
            vals[s] = jnp.zeros(vals.shape[1:], bf16)
            for h in range(kv_heads):
                bun[s, h] = jnp.zeros(bun.shape[2:], bf16)
                bun[s, h, length:2 * length] = eye.astype(bf16)

    def value_copy(kind, src, slot, to):
        return pltpu.make_async_remote_copy(
            src_ref=vals.at[src], dst_ref=vals.at[slot],
            send_sem=val_send.at[kind], recv_sem=val_recv.at[slot],
            device_id={"ctx": to}, device_id_type=MESH,
        )

    def bundle_copy(h):
        def make(kind, src, slot, to):
            return pltpu.make_async_remote_copy(
                src_ref=bun.at[src, h], dst_ref=bun.at[slot, h],
                send_sem=bun_send.at[h, kind], recv_sem=bun_recv.at[h, slot],
                device_id={"ctx": to}, device_id_type=MESH,
            )
        return make

    def stage_0(make):
        @pl.when(has_next)
        def _():
            make(0, 0, 2, ctx + 2).start()

        @pl.when(parity == 0)
        def _():
            make(1, 0, 1, partner).start()

    def stage_1(make):
        @pl.when(has_last)
        def _():
            make(0, 0, 2, partner).wait_recv()

        @pl.when(jnp.logical_and(has_last, has_next))
        def _():
            make(2, 2, 4, ctx + 2).start()

        @pl.when(jnp.logical_and(has_last, parity == 0))
        def _():
            make(3, 2, 3, partner).start()

        @pl.when(jnp.logical_and(has_last, parity == 1))
        def _():
            make(1, 2, 1, partner).start()

    def stage_2(make):
        @pl.when(ctx >= 4)
        def _():
            make(2, 0, 4, partner).wait_recv()

        @pl.when(jnp.logical_and(ctx >= 4, parity == 1))
        def _():
            make(3, 4, 3, partner).start()

    def stage_end(make):
        @pl.when(has_next)
        def _():
            make(0, 0, 2, partner).wait_send()

        @pl.when(ctx >= 2 * parity)
        def _():
            make(1, 0, 1, partner).wait_send()

        @pl.when(jnp.logical_and(has_last, has_next))
        def _():
            make(2, 0, 4, partner).wait_send()

        @pl.when(ctx >= 2 + 2 * parity)
        def _():
            make(3, 0, 3, partner).wait_send()

    def arrive(make, slot):
        @pl.when(ctx >= slot)
        def _():
            make(0, 0, slot, partner).wait_recv()

    hid_in.wait()
    b_in.wait()
    x = hid[...]
    plog[...] = lax.dot_general(
        b[...], x, (((0,), (1,)), ((), ())), preferred_element_type=f32
    )

    def part_copies(i):
        to = {"head": lax.rem(me + i, n_head)}
        return (
            pltpu.make_async_remote_copy(
                src_ref=part.at[i], dst_ref=got.at[i],
                send_sem=part_send.at[i], recv_sem=part_recv.at[i],
                device_id=to, device_id_type=MESH,
            ),
            pltpu.make_async_remote_copy(
                src_ref=plog, dst_ref=glog.at[i],
                send_sem=log_send.at[i], recv_sem=log_recv.at[i],
                device_id=to, device_id_type=MESH,
            ),
        )

    raw = None
    for n, i in enumerate(others + [0]):
        w_in[n].wait()
        term = dot(x, w[i])
        if i == 0:
            raw = term
        else:
            part[i] = term.astype(part.dtype)
            if n == 0:
                pl.semaphore_wait(
                    barrier,
                    n_head + has_next.astype(jnp.int32) + has_last.astype(jnp.int32),
                )
            for copy in part_copies(i):
                copy.start()
    v_in.wait()
    stage_0(value_copy)
    k_in.wait()
    q_in.wait()
    logit = plog[...]
    for i in others:
        for copy in part_copies(i):
            copy.wait_recv()
        raw = raw + got[i].astype(f32)
        logit = logit + glog[i]
    lsum[...] = 2.0 / (1.0 + jnp.exp(-logit))
    stage_1(value_copy)

    vec, unit, wanted, beta = [], [], [], []
    for h in range(kv_heads):
        r = raw[:, h * head_dim:(h + 1) * head_dim]
        vec.append(r * lax.rsqrt(jnp.sum(r * r, axis=-1, keepdims=True) + 1e-06))
        beta_row = lsum[pl.ds(me * kv_heads + h, 1), :]
        wide_beta = jnp.broadcast_to(beta_row, (length, length))
        beta.append(wide_beta.T)
        upper = jnp.where(row < col, mm_t(vec[h], vec[h]) * wide_beta, 0.0)
        wanted.append(upper)

    def level(size):
        return (row // (2 * size) == col // (2 * size)) & (row // size < col // size)

    unit = [eye - jnp.where(level(1), a, 0.0) for a in wanted]
    size = 2
    while size < length:
        mask = level(size)
        half = [mm(u, jnp.where(mask, a, 0.0)) for u, a in zip(unit, wanted)]
        unit = [u - mm(t, u) for u, t in zip(unit, half)]
        size *= 2

    key_low = []
    for h in range(kv_heads):
        key = k[:, h * head_dim:(h + 1) * head_dim]
        lower = jnp.where(row > col, exact_mm_t(key, vec[h]), 0.0)
        key_low.append(lower)
        y = beta[h] * mm(unit[h], vec[h])
        moved = key.astype(f32) - mm(lower, y)
        prod = eye - mm(vec[h].T, y)
        bun[0, h, 0:length] = moved.astype(bf16)
        high, low = split(prod)
        bun[0, h, length:2 * length] = high
        if PROD_PARTS == 2:
            bun[0, h, 2 * length:3 * length] = low
    for h in range(kv_heads):
        stage_0(bundle_copy(h))
    stage_2(value_copy)

    causal = jnp.concatenate([row >= col] * groups, axis=0)
    for h in range(kv_heads):
        key = k[:, h * head_dim:(h + 1) * head_dim]
        query = jnp.concatenate(
            [
                q[:, (h * groups + g) * head_dim:(h * groups + g + 1) * head_dim]
                for g in range(groups)
            ],
            axis=0,
        )
        tri = (beta[h] * unit[h]).T
        z = mm(tri, vec[h])
        mix = mm(tri, key_low[h].T)
        z_high, z_low = split(z)
        mix_high, mix_low = split(mix)
        top = jnp.concatenate([z_high, mix_high], axis=1)
        query_vec = jnp.where(causal, exact_mm_t(query, vec[h]), 0.0)
        vec_high, vec_low = split(query_vec)
        moved = dot(
            jnp.concatenate([vec_high, vec_low], axis=1), jnp.concatenate([top, top], axis=0)
        ) + dot(vec_high, jnp.concatenate([z_low, mix_low], axis=1))
        carry[h] = query.astype(f32) - moved[:, :head_dim]
        own = (dot_t(query, key) - moved[:, head_dim:]) * scaling
        score[h, 0] = jnp.where(causal, own, very_low)
        stage_1(bundle_copy(h))

    reach_now = reach[0]
    for s in range(1, STEPS):
        if s == 1:
            for h in range(kv_heads):
                arrive(bundle_copy(h), 1)
        live = jnp.logical_and(s < reach_now, ctx >= s)
        if s == 3:
            for h in range(kv_heads):
                arrive(bundle_copy(h), 3)
        for h in range(kv_heads):
            now_high, now_low = split(carry[h])
            moved = bun[s, h, 0:length]
            got_score = dot_t(now_high, moved) * scaling
            score[h, s] = jnp.where(live, got_score, very_low)
            high = bun[s, h, length:2 * length]
            now = jnp.concatenate([now_high, now_low], axis=1)
            rhs = jnp.concatenate([high, high], axis=1)
            if PROD_PARTS == 2:
                low = bun[s, h, 2 * length:3 * length]
                rhs = jnp.concatenate([rhs, jnp.concatenate([low, low], axis=1)], axis=0)
                carry[h] = halves(dot_t(now, rhs))
            else:
                carry[h] = dot_t(now, rhs)
        if s == 1:
            for h in range(kv_heads):
                stage_2(bundle_copy(h))

    arrive(value_copy, 1)
    arrive(value_copy, 3)
    lane = lax.broadcasted_iota(jnp.int32, (length, length), 1)
    stats = jnp.zeros((length, length), f32)
    n_q = kv_heads * groups
    for h in range(kv_heads):
        top = score[h, 0]
        for s in range(1, STEPS):
            top = jnp.maximum(top, score[h, s])
        top = jnp.max(top, axis=-1, keepdims=True)
        total, acc = None, None
        for s in range(STEPS):
            probs = jnp.exp(score[h, s] - top)
            value = vals[s, :, h * head_dim:(h + 1) * head_dim]
            here = dot(probs.astype(bf16), value)
            total = probs if total is None else total + probs
            acc = here if acc is None else acc + here
        total = jnp.sum(total, axis=-1, keepdims=True)
        for g in range(groups):
            rows = slice(g * length, (g + 1) * length)
            at = h * groups + g
            cols = slice(at * head_dim, (at + 1) * head_dim)
            numer[:, cols] = acc[rows]
            carried[:, cols] = carry[h, rows].astype(bf16)
            stats = jnp.where(lane == at, top[rows], stats)
            stats = jnp.where(lane == n_q + at, total[rows], stats)
    stats = stats.T
    maxima[...] = stats[:n_q]
    totals[...] = stats[n_q:2 * n_q]

    for i in others:
        for copy in part_copies(i):
            copy.wait_send()
    stage_end(value_copy)
    for h in range(kv_heads):
        stage_end(bundle_copy(h))


def solution(mesh):
    n_head, n_ctx = mesh.shape["head"], mesh.shape["ctx"]

    def body(hidden, w_proj, b_proj, queries, keys, values, reach):
        length, depth = hidden.shape
        all_heads = b_proj.shape[1]
        head_dim = w_proj.shape[1] // all_heads
        kv_heads = all_heads // n_head
        columns = kv_heads * head_dim
        n_q = queries.shape[1] // head_dim
        rows = n_q // kv_heads * length
        any_space = pl.BlockSpec(memory_space=pl.ANY)
        vmem = pl.BlockSpec(memory_space=pltpu.VMEM)
        dma = pltpu.SemaphoreType.DMA
        return pl.pallas_call(
            functools.partial(kernel, n_head, n_ctx),
            out_shape=(
                jax.ShapeDtypeStruct(queries.shape, f32),
                jax.ShapeDtypeStruct((n_q, length), f32),
                jax.ShapeDtypeStruct((n_q, length), f32),
                jax.ShapeDtypeStruct(queries.shape, bf16),
            ),
            in_specs=[any_space] * 6 + [pl.BlockSpec(memory_space=pltpu.SMEM)],
            out_specs=(vmem, vmem, vmem, vmem),
            scratch_shapes=[
                pltpu.VMEM((length, depth), bf16),
                pltpu.VMEM((n_head, depth, columns), bf16),
                pltpu.VMEM((depth, all_heads), bf16),
                pltpu.VMEM(queries.shape, bf16),
                pltpu.VMEM(keys.shape, bf16),
                pltpu.VMEM((n_head, length, columns), FAR),
                pltpu.VMEM((n_head, length, columns), FAR),
                pltpu.VMEM((all_heads, length), f32),
                pltpu.VMEM((n_head, all_heads, length), f32),
                pltpu.VMEM((all_heads, length), f32),
                pltpu.VMEM((STEPS, length, columns), bf16),
                pltpu.VMEM((STEPS, kv_heads, (1 + PROD_PARTS) * length, head_dim), bf16),
                pltpu.VMEM((kv_heads, rows, head_dim), f32),
                pltpu.VMEM((kv_heads, STEPS, rows, length), f32),
                pltpu.VMEM((8, 128), f32),
                dma((5,)),
                dma((n_head,)),
                dma((n_head,)),
                dma((n_head,)),
                dma((n_head,)),
                dma((n_head,)),
                dma((4,)),
                dma((STEPS,)),
                dma((kv_heads, 4)),
                dma((kv_heads, STEPS)),
            ],
            compiler_params=pltpu.CompilerParams(
                collective_id=0, has_side_effects=True, vmem_limit_bytes=48 << 20
            ),
        )(hidden, w_proj, b_proj, queries, keys, values, reach)

    in_specs = (
        P("ctx", "head"),
        P("head", None),
        P("head", None),
        P("ctx", "head"),
        P("ctx", "head"),
        P("ctx", "head"),
        P("ctx"),
    )
    out_specs = (P("ctx", "head"), P("head", "ctx"), P("head", "ctx"), P("ctx", "head"))
    return jax.shard_map(body, mesh=mesh, in_specs=in_specs, out_specs=out_specs, check_vma=False)
```
